32 devices in a mesh: rep: 2 (over core), row: 16 (over z, y, x).
Axes of the slice: x: 2, y: 2, z: 4, core: 2. Of those that a mesh axis runs over, the one named last changes fastest.
Arguments:
- tiles: bfloat16 [128, 16, 128, 128], P('row', 'rep'), as said below
- tile_cols: int32 [128, 16], replicated, may hold values from -1 to 127, as said below
Outputs:
- vertex_counts: float32 [128, 128], P('row', 'rep')
The draws below stay inside these ranges and needn't reach their ends.
Inputs may be any that keep to these rules, and one draw needn't show every extreme that they name: `tile_cols`: in each tile row I the filled slots come first and hold distinct tile columns from I - 32 to I, in increasing order; empty slots hold -1. At most 16 slots of a row are filled, and some row has all 16 filled. `tiles`: tiles of empty slots are zero; a tile on the diagonal (column equal to row) is zero on and above its own diagonal.
All inputs are finite; a program needn't handle non-finite values.
Results may differ from the reference program's by a relative error of at most 0.0003.
Values may be sent and summed in bfloat16 or wider, within the bound.
No kernel may reach another device: no remote copies, remote signals or barrier semaphores. Data moves between devices by JAX's collectives and lax.ppermute only.
A program may use at most 128 MiB of HBM per device.

```python
import jax
import jax.numpy as jnp
from jax import lax

TILE = 128
TR_DEV = 8
SLOTS = 16
BACK = 4
NTR = 128


def slot_columns(key):
    key = jax.random.fold_in(key, 7)
    reach = BACK * TR_DEV
    rows = jnp.arange(NTR, dtype=jnp.int32)
    lowest = jnp.minimum(1 + SLOTS * rows // NTR, SLOTS)
    filled = jnp.minimum(rows + 1, jax.random.randint(jax.random.fold_in(key, 1), (NTR,), lowest, SLOTS + 1))
    scores = jax.random.randint(jax.random.fold_in(key, 2), (NTR, NTR), 0, 1 << 20)
    colidx = jnp.arange(NTR, dtype=jnp.int32)[None, :]
    inside = (colidx <= rows[:, None]) & (colidx >= rows[:, None] - reach)
    scores = jnp.where(inside, scores, 1 << 21) * NTR + colidx
    order = jnp.argsort(scores, axis=1, stable=True)[:, :SLOTS].astype(jnp.int32)
    slot = jnp.arange(SLOTS, dtype=jnp.int32)
    chosen = jnp.where(slot[None, :] < filled[:, None], order, 2 * NTR)
    chosen = jnp.sort(chosen, axis=1)
    return jnp.where(chosen >= NTR, -1, chosen).astype(jnp.int32)


def draw_tile_cols(key, part):
    return slot_columns(key)


def draw_tiles(key, part):
    cols = slot_columns(key)
    inner = jax.random.fold_in(key, 11)
    shape = (NTR, SLOTS, TILE, TILE)
    values = jax.random.normal(inner, shape, jnp.float32)
    spread = (0.5 * SLOTS * SLOTS * TILE ** 3) ** (-1.0 / 6.0)
    values = spread * (values + 0.1)
    strict = jnp.arange(TILE)[:, None] > jnp.arange(TILE)[None, :]
    diagonal = cols == jnp.arange(NTR, dtype=jnp.int32)[:, None]
    keep = (cols >= 0)[:, :, None, None] & (jnp.logical_not(diagonal)[:, :, None, None] | strict[None, None])
    return jnp.where(keep, values, 0.0).astype(jnp.bfloat16)


def setup_inputs(seed: int = 0) -> dict:
    keys = jax.random.split(jax.random.key(seed), 3)
    tiles = draw_tiles(jax.random.fold_in(keys[2], 71), 0)
    tile_cols = draw_tile_cols(jax.random.fold_in(keys[2], 71), 0)
    return {"tiles": tiles, "tile_cols": tile_cols}


def reference(tiles, tile_cols):
    count_rows = tiles.shape[0]

    def per_row(index):
        cols = tile_cols[index]
        mine = tiles[index].astype(jnp.float32)
        safe = jnp.maximum(cols, 0).astype(jnp.int32)
        panels = tiles[safe].astype(jnp.float32)
        panel_cols = tile_cols[safe]
        match = (panel_cols[:, :, None] == cols[None, None, :]) & (cols >= 0)[None, None, :]
        masks = jnp.einsum("kjp,pac->kjac", match.astype(jnp.float32), mine, precision=lax.Precision.HIGHEST)
        product = jnp.einsum("kab,kjbc->kjac", mine, panels, precision=lax.Precision.HIGHEST)
        return jnp.sum(product * masks, axis=(0, 1, 3))

    return lax.map(per_row, jnp.arange(count_rows, dtype=jnp.int32))
```

```python
import jax
import jax.numpy as jnp
from jax import lax
from jax.experimental import pallas as pl
from jax.experimental.pallas import tpu as pltpu
from jax.sharding import PartitionSpec as P

BACK = 4
UNROLL = 8
OWN, SIDE, NEXT, UP3, UP, SIDE_NEXT, SIDE_UP, NEXT_UP, UP3_DIAG, UP_DOWN = range(10)
GROUPS = 10
ARRIVES = (
    (UP3_DIAG, NEXT_UP, UP_DOWN, UP),
    (SIDE, NEXT_UP, UP_DOWN, UP),
    (SIDE_NEXT, NEXT, SIDE_UP, UP),
    (SIDE, NEXT, SIDE_NEXT, UP3),
)


def swap_cores(x):
    return lax.ppermute(x, "rep", [(0, 1), (1, 0)])


def moved(x, steps):
    size = lax.axis_size("row")
    route = [(i, i + steps[i % BACK]) for i in range(size) if i % BACK in steps]
    return lax.ppermute(x, "row", [(i, j) for i, j in route if j < size])


def running(flags):
    n = flags.shape[-1]
    tri = (jnp.arange(n)[:, None] < jnp.arange(n)[None, :]).astype(jnp.bfloat16)
    flat = flags.reshape(-1, n).astype(jnp.bfloat16)
    count = jnp.dot(flat, tri, preferred_element_type=jnp.float32)
    return count.astype(jnp.int32).reshape(flags.shape)


def send_lists(tile_cols, rows):
    count, slots = tile_cols.shape
    blocks = count // rows
    every = jnp.arange(count, dtype=jnp.int32)
    hot = tile_cols[:, :, None] == every
    member = jnp.any(hot, axis=1).astype(jnp.bfloat16).reshape(blocks, rows, count)
    padded = jnp.pad(member, ((0, BACK), (0, 0), (0, 0)))
    later = jnp.concatenate([padded[d : d + blocks] for d in range(1, BACK + 1)], axis=1)
    column = hot.reshape(blocks, rows * slots, count).astype(jnp.bfloat16)
    line = jnp.broadcast_to((every[:, None] == every)[:, None, :], hot.shape)
    line = line.reshape(blocks, rows * slots, count).astype(jnp.bfloat16)
    dims = (((2,), (2,)), ((0,), (0,)))
    has_column = lax.dot_general(later, column, dims, preferred_element_type=jnp.float32)
    has_line = lax.dot_general(later, line, dims, preferred_element_type=jnp.float32)
    both = (has_column * has_line).reshape(blocks, BACK, rows, rows * slots)
    need = jnp.max(both, axis=2) > 0
    place = (jnp.arange(blocks) % BACK)[:, None]
    near, second, third, fourth = (need[:, d] for d in range(BACK))
    side = (near & (place != 3)) | (third & ((place == 0) | (place == 3)))
    upper = fourth | (near & (place == 3)) | (third & ((place == 1) | (place == 2)))
    return jnp.stack([side, second, upper], axis=1)


def gather_kernel(caps, lists, index_ref, mine_ref, other_ref, *rest):
    outs, pool, sem = rest[:-2], rest[-2], rest[-1]
    half = mine_ref.shape[0]
    first = pltpu.make_async_copy(mine_ref, pool.at[pl.ds(0, half)], sem.at[0])
    second = pltpu.make_async_copy(other_ref, pool.at[pl.ds(half, half)], sem.at[1])
    first.start()
    second.start()
    first.wait()
    second.wait()
    for out, cap, which in zip(outs, caps, lists):

        def one(p, carry, out=out, which=which):
            out[p] = pool[index_ref[which, p]]
            return carry

        lax.fori_loop(0, cap, one, 0, unroll=2)


def gather_tiles(caps, lists, index, mine, other):
    tile = mine.shape[-2:]
    anywhere = pl.BlockSpec(memory_space=pl.ANY)
    return pl.pallas_call(
        lambda *refs: gather_kernel(caps, lists, *refs),
        out_shape=[jax.ShapeDtypeStruct((cap,) + tile, mine.dtype) for cap in caps],
        in_specs=[pl.BlockSpec(memory_space=pltpu.SMEM), anywhere, anywhere],
        out_specs=[pl.BlockSpec(memory_space=pltpu.VMEM)] * len(caps),
        scratch_shapes=[
            pltpu.VMEM((2 * mine.shape[0],) + tile, mine.dtype),
            pltpu.SemaphoreType.DMA((2,)),
        ],
        cost_estimate=pl.CostEstimate(
            flops=10**6, bytes_accessed=sum(caps) * 65536, transcendentals=0
        ),
    )(index, mine, other)


def count_kernel(groups, rows, start_ref, item_ref, before_ref, mine_ref, other_ref, *rest):
    n = len(groups)
    bufs, out_ref, own, acc = rest[:n], rest[n], rest[n + 1], rest[n + 2]
    held, sem, own_sem = rest[n + 3 : 2 * n + 3], rest[-2], rest[-1]
    half = mine_ref.shape[0]
    slots_here = half // rows
    first = pltpu.make_async_copy(mine_ref, own.at[pl.ds(0, half)], own_sem.at[0])
    second = pltpu.make_async_copy(other_ref, own.at[pl.ds(half, half)], own_sem.at[1])
    first.start()
    second.start()
    for i, group in enumerate(groups):

        @pl.when(start_ref[group + 1] > start_ref[group])
        def _(i=i):
            pltpu.make_async_copy(bufs[i], held[i], sem.at[i]).start()

    own[2 * half] = jnp.zeros(own.shape[1:], own.dtype)
    acc[...] = jnp.zeros_like(acc)
    first.wait()
    second.wait()

    def work(group, source):
        def step(i, carry):
            for u in range(UNROLL):
                code = item_ref[i * UNROLL + u]
                a = code & 255
                b = (code >> 8) & 255
                t = code >> 16
                row = (a & (half - 1)) // slots_here
                product = jnp.dot(own[a], source[t], preferred_element_type=jnp.float32)
                acc[row] += product * own[b].astype(jnp.float32)
            return carry

        lax.fori_loop(start_ref[group], start_ref[group + 1], step, 0)

    if not groups:
        work(OWN, own)
    for i, group in enumerate(groups):

        @pl.when(start_ref[group + 1] > start_ref[group])
        def _(i=i, group=group):
            pltpu.make_async_copy(bufs[i], held[i], sem.at[i]).wait()
            work(group, held[i])

    out_ref[...] = before_ref[...] + jnp.sum(acc[...], axis=2)


def count_tiles(groups, rows, starts, items, before, mine, other, bufs, flops):
    half, tile, _ = mine.shape
    anywhere = pl.BlockSpec(memory_space=pl.ANY)
    vmem = pl.BlockSpec(memory_space=pltpu.VMEM)
    return pl.pallas_call(
        lambda *refs: count_kernel(groups, rows, *refs),
        out_shape=jax.ShapeDtypeStruct((rows, tile), jnp.float32),
        in_specs=[pl.BlockSpec(memory_space=pltpu.SMEM)] * 2 + [vmem] + [anywhere] * (2 + len(bufs)),
        out_specs=vmem,
        scratch_shapes=[
            pltpu.VMEM((2 * half + 1, tile, tile), mine.dtype),
            pltpu.VMEM((rows, tile, tile), jnp.float32),
        ]
        + [pltpu.VMEM(b.shape, b.dtype) for b in bufs]
        + [pltpu.SemaphoreType.DMA((max(1, len(bufs)),)), pltpu.SemaphoreType.DMA((2,))],
        cost_estimate=pl.CostEstimate(flops=flops, bytes_accessed=8 * 10**6, transcendentals=0),
    )(starts, items, before, mine, other, *bufs)


def work_items(tile_cols, lists, ranks, rows, half_slots, here, core, loc):
    count, slots = tile_cols.shape
    per_block = rows * slots
    half = rows * half_slots
    place = here % BACK
    window = (BACK + 1) * rows

    pad = ((BACK, 0), (0, 0), (0, 0))
    near_lists = lax.dynamic_slice_in_dim(jnp.pad(lists, pad), here, BACK, 0)
    near_ranks = lax.dynamic_slice_in_dim(jnp.pad(ranks, pad), here, BACK, 0)
    from_place = (here + jnp.arange(BACK)) % BACK
    dist = BACK - jnp.arange(BACK)
    upper = (dist == 4) | ((dist == 1) & (from_place == 3))
    upper = upper | ((dist == 3) & ((from_place == 1) | (from_place == 2)))
    which = jnp.where(dist == 2, 1, jnp.where(upper, 2, 0))
    pick = (which[:, None] == jnp.arange(3))[:, :, None]
    flag = jnp.any(near_lists & pick, axis=1)
    rank = jnp.sum(jnp.where(pick, near_ranks, 0), axis=1)
    spot = jnp.where(flag & (rank % 2 == core), rank // 2 + 1, 0)
    order = jnp.arange(per_block, dtype=jnp.int32)
    own_spot = jnp.where(order % 2 == core, loc + 1, 0)
    spot = jnp.concatenate([spot, own_spot[None]], axis=0)

    base = (here - BACK) * rows
    inside = jnp.arange(window, dtype=jnp.int32)
    padded = jnp.pad(tile_cols, ((BACK * rows, 0), (0, 0)), constant_values=-1)
    near = lax.dynamic_slice(padded, (here * rows, 0), (window, slots))
    hot = (near[:, :, None] - base == inside) & (near >= 0)[:, :, None]
    table = spot.reshape(window, slots)
    table = jnp.sum(jnp.where(hot, table[:, :, None], 0), axis=1).astype(jnp.bfloat16)
    mine_hot = hot[BACK * rows :].astype(jnp.bfloat16)
    found = jnp.einsum("ipk,kj->ipj", mine_hot, table, preferred_element_type=jnp.float32)
    found = jnp.einsum(
        "ipj,iqj->ipq", found.astype(jnp.bfloat16), mine_hot, preferred_element_type=jnp.float32
    ).astype(jnp.int32)
    my_cols = near[BACK * rows :]
    back = here - my_cols // rows
    group = jnp.zeros_like(back)
    for row in range(BACK):
        for d in range(1, BACK + 1):
            group = jnp.where((place == row) & (back == d), ARRIVES[row][d - 1], group)
    own_loc = loc.reshape(rows, slots)
    code = own_loc[:, :, None] + own_loc[:, None, :] * 256 + (found - 1) * 65536
    total = rows * slots * slots
    valid = (found > 0).reshape(total // 128, 128)
    group = jnp.broadcast_to(group[:, :, None], (rows, slots, slots)).reshape(total // 128, 128)
    ids = jnp.arange(GROUPS, dtype=jnp.int32)
    chosen = (group == ids[:, None, None]) & valid
    lane_rank = running(chosen)
    lane_sum = jnp.sum(chosen.astype(jnp.int32), axis=2)
    major = running(lane_sum)
    trips = (jnp.sum(lane_sum, axis=1) + UNROLL - 1) // UNROLL
    starts = jnp.sum(jnp.where(jnp.arange(GROUPS + 1)[:, None] > ids, trips, 0), axis=1)
    spread = lane_rank + (major + starts[:GROUPS, None] * UNROLL + 1)[:, :, None]
    target = jnp.sum(jnp.where(chosen, spread, 0), axis=0).reshape(1, total)
    dummy = 256 * 2 * half
    limit = rows * slots * (slots + 1) // 2 + GROUPS * UNROLL
    limit = -(-limit // 128) * 128
    at = jnp.arange(1, limit + 1, dtype=jnp.int32)[:, None]
    hit = jnp.where(target == at, code.reshape(1, total) - dummy, 0)
    return starts, dummy + jnp.sum(hit, axis=1)


def body(tiles, tile_cols):
    rows, half_slots, tile, _ = tiles.shape
    count, slots = tile_cols.shape
    core = lax.axis_index("rep")
    here = lax.axis_index("row")
    half = rows * half_slots
    per_block = rows * slots
    mine = tiles.reshape(half, tile, tile)
    other = swap_cores(mine)

    lists = send_lists(tile_cols, rows)
    ranks = running(lists)
    totals = jnp.sum(lists.astype(jnp.int32), axis=2)
    slot = jnp.arange(per_block, dtype=jnp.int32)
    line, column = slot // slots, slot % slots
    loc = ((column // half_slots) ^ core) * half + line * half_slots + column % half_slots

    full = per_block // 2
    my_list = lax.dynamic_index_in_dim(lists, here, 0, False)
    my_rank = lax.dynamic_index_in_dim(ranks, here, 0, False)
    want = (jnp.arange(full, dtype=jnp.int32) * 2 + core)[None, :, None]
    match = my_list[:, None, :] & (my_rank[:, None, :] == want)
    index = jnp.sum(jnp.where(match, loc, 0), axis=2)

    starts, items = work_items(tile_cols, lists, ranks, rows, half_slots, here, core, loc)

    def run(caps):
        side_cap, next_cap, up3_cap, up_cap = caps

        def exchange(mine, other, index, starts, items):
            side, second, up3, up = gather_tiles(caps, (0, 1, 2, 2), index, mine, other)
            side = moved(side, {0: 1, 1: -1, 2: 1, 3: -1})
            up3 = moved(up3, {3: 4})
            second = moved(second, {0: 2, 1: 2, 2: -2, 3: -2})
            up = moved(up, {0: 4, 1: 4, 2: 4})
            side_next = moved(side, {0: 2, 1: 2})
            side_up = moved(side, {2: 4})
            up3_diag = moved(up3, {3: -3})
            next_up = moved(second, {0: 4, 1: 4})
            up_down = moved(up, {1: -1, 2: -1})
            counts = jnp.zeros((rows, tile), jnp.float32)
            counts = count_tiles((), rows, starts, items, counts, mine, other, [], 10**9)
            counts = count_tiles(
                (SIDE, NEXT, UP3, UP), rows, starts, items, counts, mine, other,
                [side, second, up3, up], 2 * 10**9,
            )
            return count_tiles(
                (SIDE_NEXT, SIDE_UP, NEXT_UP, UP3_DIAG, UP_DOWN), rows, starts, items, counts,
                mine, other, [side_next, side_up, next_up, up3_diag, up_down], 2 * 10**9,
            )

        return exchange

    brief = (full * 3 // 4, full * 5 // 8, full * 11 // 16, full * 15 // 32)
    place = jnp.arange(totals.shape[0]) % BACK
    bound = jnp.stack(
        [
            jnp.full_like(place, 2 * brief[0]),
            jnp.full_like(place, 2 * brief[1]),
            jnp.where(place == 3, 2 * brief[2], 2 * brief[3]),
        ],
        axis=1,
    )
    fits = jnp.all(totals <= bound)
    partial = lax.cond(fits, run(brief), run((full,) * 4), mine, other, index, starts, items)

    width = tile // 2
    keep = lax.dynamic_slice_in_dim(partial, core * width, width, 1)
    give = lax.dynamic_slice_in_dim(partial, (1 - core) * width, width, 1)
    return keep + swap_cores(give)


def solution(mesh):
    return jax.shard_map(
        body,
        mesh=mesh,
        in_specs=(P("row", "rep", None, None), P()),
        out_specs=P("row", "rep"),
        check_vma=False,
    )
```

```python
import jax
import jax.numpy as jnp
from jax import lax
from jax.experimental import pallas as pl
from jax.experimental.pallas import tpu as pltpu
from jax.sharding import PartitionSpec as P

BACK = 4
UNROLL = 8
(OWN, SIDE0, SIDE1, NEXT, UP3, UP) = range(6)
(SIDE_NEXT0, SIDE_NEXT1, SIDE_UP, NEXT_UP, UP3_DIAG, UP_DOWN) = range(6, 12)
GROUPS = 12
SPLIT = (SIDE0, SIDE_NEXT0)
ARRIVES = (
    (UP3_DIAG, NEXT_UP, UP_DOWN, UP),
    (SIDE0, NEXT_UP, UP_DOWN, UP),
    (SIDE_NEXT0, NEXT, SIDE_UP, UP),
    (SIDE0, NEXT, SIDE_NEXT0, UP3),
)


def swap_cores(x):
    return lax.ppermute(x, "rep", [(0, 1), (1, 0)])


def moved(x, steps):
    size = lax.axis_size("row")
    route = [(i, i + steps[i % BACK]) for i in range(size) if i % BACK in steps]
    return lax.ppermute(x, "row", [(i, j) for i, j in route if j < size])


def running(flags):
    n = flags.shape[-1]
    tri = (jnp.arange(n)[:, None] < jnp.arange(n)[None, :]).astype(jnp.bfloat16)
    flat = flags.reshape(-1, n).astype(jnp.bfloat16)
    count = jnp.dot(flat, tri, preferred_element_type=jnp.float32)
    return count.astype(jnp.int32).reshape(flags.shape)


def send_lists(tile_cols, rows):
    count, slots = tile_cols.shape
    blocks = count // rows
    every = jnp.arange(count, dtype=jnp.int32)
    hot = tile_cols[:, :, None] == every
    member = jnp.any(hot, axis=1).astype(jnp.bfloat16).reshape(blocks, rows, count)
    padded = jnp.pad(member, ((0, BACK), (0, 0), (0, 0)))
    later = jnp.concatenate([padded[d : d + blocks] for d in range(1, BACK + 1)], axis=1)
    column = hot.reshape(blocks, rows * slots, count).astype(jnp.bfloat16)
    line = jnp.broadcast_to((every[:, None] == every)[:, None, :], hot.shape)
    line = line.reshape(blocks, rows * slots, count).astype(jnp.bfloat16)
    dims = (((2,), (2,)), ((0,), (0,)))
    has_column = lax.dot_general(later, column, dims, preferred_element_type=jnp.float32)
    has_line = lax.dot_general(later, line, dims, preferred_element_type=jnp.float32)
    both = (has_column * has_line).reshape(blocks, BACK, rows, rows * slots)
    need = jnp.max(both, axis=2) > 0
    place = (jnp.arange(blocks) % BACK)[:, None]
    near, second, third, fourth = (need[:, d] for d in range(BACK))
    side = (near & (place != 3)) | (third & ((place == 0) | (place == 3)))
    upper = fourth | (near & (place == 3)) | (third & ((place == 1) | (place == 2)))
    lists = jnp.stack([side, second, upper], axis=1)
    ahead = side & third & ((place == 0) | (place == 3))
    order = running(jnp.concatenate([lists, ahead[:, None]], axis=1))
    first = order[:, 3]
    total = jnp.sum(ahead.astype(jnp.int32), axis=1, keepdims=True)
    side_rank = jnp.where(ahead, first, order[:, 0] - first + total)
    ranks = jnp.concatenate([side_rank[:, None], order[:, 1:3]], axis=1)
    return lists, ranks, total[:, 0]


def gather_kernel(pieces, index_ref, mine_ref, other_ref, *rest):
    outs, pool, sem = rest[:-2], rest[-2], rest[-1]
    half = mine_ref.shape[0]
    first = pltpu.make_async_copy(mine_ref, pool.at[pl.ds(0, half)], sem.at[0])
    second = pltpu.make_async_copy(other_ref, pool.at[pl.ds(half, half)], sem.at[1])
    first.start()
    second.start()
    first.wait()
    second.wait()
    for out, (which, start, cap) in zip(outs, pieces):

        def one(p, carry, out=out, which=which, start=start):
            out[p] = pool[index_ref[which, start + p]]
            return carry

        lax.fori_loop(0, cap, one, 0, unroll=2)


def gather_tiles(pieces, index, mine, other):
    tile = mine.shape[-2:]
    anywhere = pl.BlockSpec(memory_space=pl.ANY)
    total = sum(cap for _, _, cap in pieces)
    return pl.pallas_call(
        lambda *refs: gather_kernel(pieces, *refs),
        out_shape=[jax.ShapeDtypeStruct((cap,) + tile, mine.dtype) for _, _, cap in pieces],
        in_specs=[pl.BlockSpec(memory_space=pltpu.SMEM), anywhere, anywhere],
        out_specs=[pl.BlockSpec(memory_space=pltpu.VMEM)] * len(pieces),
        scratch_shapes=[
            pltpu.VMEM((2 * mine.shape[0],) + tile, mine.dtype),
            pltpu.SemaphoreType.DMA((2,)),
        ],
        cost_estimate=pl.CostEstimate(
            flops=10**6, bytes_accessed=total * 65536, transcendentals=0
        ),
    )(index, mine, other)


def count_kernel(groups, rows, start_ref, item_ref, before_ref, mine_ref, other_ref, *rest):
    n = len(groups)
    bufs, out_ref, own, acc = rest[:n], rest[n], rest[n + 1], rest[n + 2]
    held, sem, own_sem = rest[n + 3 : 2 * n + 3], rest[-2], rest[-1]
    half = mine_ref.shape[0]
    slots_here = half // rows
    first = pltpu.make_async_copy(mine_ref, own.at[pl.ds(0, half)], own_sem.at[0])
    second = pltpu.make_async_copy(other_ref, own.at[pl.ds(half, half)], own_sem.at[1])
    first.start()
    second.start()
    for i, group in enumerate(groups):

        @pl.when(start_ref[group + 1] > start_ref[group])
        def _(i=i):
            pltpu.make_async_copy(bufs[i], held[i], sem.at[i]).start()

    own[2 * half] = jnp.zeros(own.shape[1:], own.dtype)
    acc[...] = jnp.zeros_like(acc)
    first.wait()
    second.wait()

    def work(group, source):
        def step(i, carry):
            for u in range(UNROLL):
                code = item_ref[i * UNROLL + u]
                a = code & 255
                b = (code >> 8) & 255
                t = code >> 16
                row = (a & (half - 1)) // slots_here
                product = jnp.dot(own[a], source[t], preferred_element_type=jnp.float32)
                acc[row] += product * own[b].astype(jnp.float32)
            return carry

        lax.fori_loop(start_ref[group], start_ref[group + 1], step, 0)

    if not groups:
        work(OWN, own)
    for i, group in enumerate(groups):

        @pl.when(start_ref[group + 1] > start_ref[group])
        def _(i=i, group=group):
            pltpu.make_async_copy(bufs[i], held[i], sem.at[i]).wait()
            work(group, held[i])

    out_ref[...] = before_ref[...] + jnp.sum(acc[...], axis=2)


def count_tiles(groups, rows, starts, items, before, mine, other, bufs, flops):
    half, tile, _ = mine.shape
    anywhere = pl.BlockSpec(memory_space=pl.ANY)
    vmem = pl.BlockSpec(memory_space=pltpu.VMEM)
    return pl.pallas_call(
        lambda *refs: count_kernel(groups, rows, *refs),
        out_shape=jax.ShapeDtypeStruct((rows, tile), jnp.float32),
        in_specs=[pl.BlockSpec(memory_space=pltpu.SMEM)] * 2 + [vmem] + [anywhere] * (2 + len(bufs)),
        out_specs=vmem,
        scratch_shapes=[
            pltpu.VMEM((2 * half + 1, tile, tile), mine.dtype),
            pltpu.VMEM((rows, tile, tile), jnp.float32),
        ]
        + [pltpu.VMEM(b.shape, b.dtype) for b in bufs]
        + [pltpu.SemaphoreType.DMA((max(1, len(bufs)),)), pltpu.SemaphoreType.DMA((2,))],
        cost_estimate=pl.CostEstimate(flops=flops, bytes_accessed=8 * 10**6, transcendentals=0),
    )(starts, items, before, mine, other, *bufs)


def work_items(tile_cols, lists, ranks, rows, half_slots, here, core, loc, cut):
    count, slots = tile_cols.shape
    per_block = rows * slots
    half = rows * half_slots
    place = here % BACK
    window = (BACK + 1) * rows

    pad = ((BACK, 0), (0, 0), (0, 0))
    near_lists = lax.dynamic_slice_in_dim(jnp.pad(lists, pad), here, BACK, 0)
    near_ranks = lax.dynamic_slice_in_dim(jnp.pad(ranks, pad), here, BACK, 0)
    from_place = (here + jnp.arange(BACK)) % BACK
    dist = BACK - jnp.arange(BACK)
    upper = (dist == 4) | ((dist == 1) & (from_place == 3))
    upper = upper | ((dist == 3) & ((from_place == 1) | (from_place == 2)))
    which = jnp.where(dist == 2, 1, jnp.where(upper, 2, 0))
    pick = (which[:, None] == jnp.arange(3))[:, :, None]
    flag = jnp.any(near_lists & pick, axis=1)
    rank = jnp.sum(jnp.where(pick, near_ranks, 0), axis=1)
    spot = jnp.where(flag & (rank % 2 == core), rank // 2 + 1, 0)
    order = jnp.arange(per_block, dtype=jnp.int32)
    own_spot = jnp.where(order % 2 == core, loc + 1, 0)
    spot = jnp.concatenate([spot, own_spot[None]], axis=0)

    base = (here - BACK) * rows
    inside = jnp.arange(window, dtype=jnp.int32)
    padded = jnp.pad(tile_cols, ((BACK * rows, 0), (0, 0)), constant_values=-1)
    near = lax.dynamic_slice(padded, (here * rows, 0), (window, slots))
    hot = (near[:, :, None] - base == inside) & (near >= 0)[:, :, None]
    table = spot.reshape(window, slots)
    table = jnp.sum(jnp.where(hot, table[:, :, None], 0), axis=1).astype(jnp.bfloat16)
    mine_hot = hot[BACK * rows :].astype(jnp.bfloat16)
    found = jnp.einsum("ipk,kj->ipj", mine_hot, table, preferred_element_type=jnp.float32)
    found = jnp.einsum(
        "ipj,iqj->ipq", found.astype(jnp.bfloat16), mine_hot, preferred_element_type=jnp.float32
    ).astype(jnp.int32)
    my_cols = near[BACK * rows :]
    back = here - my_cols // rows
    group = jnp.zeros_like(back)
    for row in range(BACK):
        for d in range(1, BACK + 1):
            group = jnp.where((place == row) & (back == d), ARRIVES[row][d - 1], group)
    group = jnp.broadcast_to(group[:, :, None], (rows, slots, slots))
    later = found > cut
    for split in SPLIT:
        second = (group == split) & later
        group = jnp.where(second, split + 1, group)
        found = jnp.where(second, found - cut, found)
    own_loc = loc.reshape(rows, slots)
    code = own_loc[:, :, None] + own_loc[:, None, :] * 256 + (found - 1) * 65536
    total = rows * slots * slots
    valid = (found > 0).reshape(total // 128, 128)
    group = group.reshape(total // 128, 128)
    ids = jnp.arange(GROUPS, dtype=jnp.int32)
    chosen = (group == ids[:, None, None]) & valid
    lane_rank = running(chosen)
    lane_sum = jnp.sum(chosen.astype(jnp.int32), axis=2)
    major = running(lane_sum)
    trips = (jnp.sum(lane_sum, axis=1) + UNROLL - 1) // UNROLL
    starts = jnp.sum(jnp.where(jnp.arange(GROUPS + 1)[:, None] > ids, trips, 0), axis=1)
    spread = lane_rank + (major + starts[:GROUPS, None] * UNROLL + 1)[:, :, None]
    target = jnp.sum(jnp.where(chosen, spread, 0), axis=0).reshape(1, total)
    dummy = 256 * 2 * half
    limit = rows * slots * (slots + 1) // 2 + GROUPS * UNROLL
    limit = -(-limit // 128) * 128
    at = jnp.arange(1, limit + 1, dtype=jnp.int32)[:, None]
    hit = jnp.where(target == at, code.reshape(1, total) - dummy, 0)
    return starts, dummy + jnp.sum(hit, axis=1)


def body(tiles, tile_cols):
    rows, half_slots, tile, _ = tiles.shape
    count, slots = tile_cols.shape
    core = lax.axis_index("rep")
    here = lax.axis_index("row")
    half = rows * half_slots
    per_block = rows * slots
    mine = tiles.reshape(half, tile, tile)
    other = swap_cores(mine)

    lists, ranks, ahead = send_lists(tile_cols, rows)
    totals = jnp.sum(lists.astype(jnp.int32), axis=2)
    slot = jnp.arange(per_block, dtype=jnp.int32)
    line, column = slot // slots, slot % slots
    loc = ((column // half_slots) ^ core) * half + line * half_slots + column % half_slots

    full = per_block // 2
    my_list = lax.dynamic_index_in_dim(lists, here, 0, False)
    my_rank = lax.dynamic_index_in_dim(ranks, here, 0, False)
    want = (jnp.arange(full, dtype=jnp.int32) * 2 + core)[None, :, None]
    match = my_list[:, None, :] & (my_rank[:, None, :] == want)
    index = jnp.sum(jnp.where(match, loc, 0), axis=2)

    def run(caps):
        cut, rest = caps[0], caps[1]

        def exchange(mine, other, index, tile_cols, lists, ranks):
            pieces = [(0, 0, cut), (1, 0, caps[2]), (2, 0, caps[3]), (2, 0, caps[4])]
            pieces += [(0, cut, rest)] * (rest > 0)
            sent = gather_tiles(pieces, index, mine, other)
            sent, tile_cols, lists, ranks = lax.optimization_barrier(
                (sent, tile_cols, lists, ranks)
            )
            side0 = moved(sent[0], {0: 1, 1: -1, 2: 1, 3: -1})
            up3 = moved(sent[2], {3: 4})
            second = moved(sent[1], {0: 2, 1: 2, 2: -2, 3: -2})
            up = moved(sent[3], {0: 4, 1: 4, 2: 4})
            side_next0 = moved(side0, {0: 2, 1: 2})
            side_up = moved(side0, {2: 4})
            next_up = moved(second, {0: 4, 1: 4})
            up3_diag = moved(up3, {3: -3})
            up_down = moved(up, {1: -1, 2: -1})
            early = {SIDE0: side0, NEXT: second, UP3: up3, UP: up}
            middle = {SIDE_NEXT0: side_next0, SIDE_UP: side_up, NEXT_UP: next_up, UP_DOWN: up_down}
            late = {UP3_DIAG: up3_diag}
            if rest:
                early[SIDE1] = moved(sent[4], {0: 1, 1: -1, 2: 1, 3: -1})
                late[SIDE_NEXT1] = moved(early[SIDE1], {0: 2})
            starts, items = work_items(
                tile_cols, lists, ranks, rows, half_slots, here, core, loc, cut
            )
            counts = jnp.zeros((rows, tile), jnp.float32)
            counts = count_tiles((), rows, starts, items, counts, mine, other, [], 10**9)
            for bufs in (early, middle, late):
                counts = count_tiles(
                    tuple(bufs), rows, starts, items, counts, mine, other, list(bufs.values()), 10**9
                )
            return counts

        return exchange

    place = jnp.arange(totals.shape[0]) % BACK

    def fit(caps):
        upper = jnp.where(place == 3, caps[3], caps[4])
        sizes = jnp.stack([ahead, totals[:, 0], totals[:, 1], totals[:, 2]], axis=1)
        bound = [jnp.full_like(place, c) for c in (caps[0], caps[0] + caps[1], caps[2])] + [upper]
        return jnp.all(sizes <= 2 * jnp.stack(bound, axis=1))

    brief = (full * 7 // 16, full * 5 // 16, full * 5 // 8, full * 11 // 16, full * 15 // 32)
    most = (full, 0, full, full, full)
    partial = lax.cond(
        fit(brief), run(brief), run(most), mine, other, index, tile_cols, lists, ranks
    )

    width = tile // 2
    keep = lax.dynamic_slice_in_dim(partial, core * width, width, 1)
    give = lax.dynamic_slice_in_dim(partial, (1 - core) * width, width, 1)
    return keep + swap_cores(give)


def solution(mesh):
    return jax.shard_map(
        body,
        mesh=mesh,
        in_specs=(P("row", "rep", None, None), P()),
        out_specs=P("row", "rep"),
        check_vma=False,
    )
```

```python
import jax
import jax.numpy as jnp
from jax import lax
from jax.experimental import pallas as pl
from jax.experimental.pallas import tpu as pltpu
from jax.sharding import PartitionSpec as P


BACK = 4
UNROLL = 8
(OWN, SIDE0, SIDE1, NEXT, UP3, UP) = range(6)
(SIDE_NEXT0, SIDE_NEXT1, SIDE_UP, NEXT_UP, UP3_DIAG, UP_DOWN) = range(6, 12)
GROUPS = 12
SPLIT = (SIDE0, SIDE_NEXT0)
ARRIVES = (
    (UP3_DIAG, NEXT_UP, UP_DOWN, UP),
    (SIDE0, NEXT_UP, UP_DOWN, UP),
    (SIDE_NEXT0, NEXT, SIDE_UP, UP),
    (SIDE0, NEXT, SIDE_NEXT0, UP3),
)


def swap_cores(x):
    return lax.ppermute(x, "rep", [(0, 1), (1, 0)])


def moved(x, steps):
    size = lax.axis_size("row")
    route = [(i, i + steps[i % BACK]) for i in range(size) if i % BACK in steps]
    return lax.ppermute(x, "row", [(i, j) for i, j in route if j < size])


def running(flags):
    n = flags.shape[-1]
    tri = (jnp.arange(n)[:, None] < jnp.arange(n)[None, :]).astype(jnp.bfloat16)
    flat = flags.reshape(-1, n).astype(jnp.bfloat16)
    count = jnp.dot(flat, tri, preferred_element_type=jnp.float32)
    return count.astype(jnp.int32).reshape(flags.shape)


def send_lists(tile_cols, rows):
    count, slots = tile_cols.shape
    blocks = count // rows
    every = jnp.arange(count, dtype=jnp.int32)
    hot = tile_cols[:, :, None] == every
    member = jnp.any(hot, axis=1).astype(jnp.bfloat16).reshape(blocks, rows, count)
    padded = jnp.pad(member, ((0, BACK), (0, 0), (0, 0)))
    later = jnp.concatenate([padded[d : d + blocks] for d in range(1, BACK + 1)], axis=1)
    column = hot.reshape(blocks, rows * slots, count).astype(jnp.bfloat16)
    line = jnp.broadcast_to((every[:, None] == every)[:, None, :], hot.shape)
    line = line.reshape(blocks, rows * slots, count).astype(jnp.bfloat16)
    dims = (((2,), (2,)), ((0,), (0,)))
    has_column = lax.dot_general(later, column, dims, preferred_element_type=jnp.float32)
    has_line = lax.dot_general(later, line, dims, preferred_element_type=jnp.float32)
    both = (has_column * has_line).reshape(blocks, BACK, rows, rows * slots)
    need = jnp.max(both, axis=2) > 0
    place = (jnp.arange(blocks) % BACK)[:, None]
    near, second, third, fourth = (need[:, d] for d in range(BACK))
    side = (near & (place != 3)) | (third & ((place == 0) | (place == 3)))
    upper = fourth | (near & (place == 3)) | (third & ((place == 1) | (place == 2)))
    lists = jnp.stack([side, second, upper], axis=1)
    ahead = side & third & ((place == 0) | (place == 3))
    order = running(jnp.concatenate([lists, ahead[:, None]], axis=1))
    first = order[:, 3]
    total = jnp.sum(ahead.astype(jnp.int32), axis=1, keepdims=True)
    side_rank = jnp.where(ahead, first, order[:, 0] - first + total)
    ranks = jnp.concatenate([side_rank[:, None], order[:, 1:3]], axis=1)
    return lists, ranks, total[:, 0]


def gather_kernel(pieces, index_ref, mine_ref, other_ref, *rest):
    outs, pool, sem = rest[:-2], rest[-2], rest[-1]
    half = mine_ref.shape[0]
    first = pltpu.make_async_copy(mine_ref, pool.at[pl.ds(0, half)], sem.at[0])
    second = pltpu.make_async_copy(other_ref, pool.at[pl.ds(half, half)], sem.at[1])
    first.start()
    second.start()
    first.wait()
    second.wait()
    for out, (which, start, cap) in zip(outs, pieces):

        def one(p, carry, out=out, which=which, start=start):
            out[p] = pool[index_ref[which, start + p]]
            return carry

        lax.fori_loop(0, cap, one, 0, unroll=2)


def gather_tiles(pieces, index, mine, other):
    tile = mine.shape[-2:]
    anywhere = pl.BlockSpec(memory_space=pl.ANY)
    total = sum(cap for _, _, cap in pieces)
    return pl.pallas_call(
        lambda *refs: gather_kernel(pieces, *refs),
        out_shape=[jax.ShapeDtypeStruct((cap,) + tile, mine.dtype) for _, _, cap in pieces],
        in_specs=[pl.BlockSpec(memory_space=pltpu.SMEM), anywhere, anywhere],
        out_specs=[pl.BlockSpec(memory_space=pltpu.VMEM)] * len(pieces),
        scratch_shapes=[
            pltpu.VMEM((2 * mine.shape[0],) + tile, mine.dtype),
            pltpu.SemaphoreType.DMA((2,)),
        ],
        cost_estimate=pl.CostEstimate(
            flops=10**6, bytes_accessed=total * 65536, transcendentals=0
        ),
    )(index, mine, other)


def count_kernel(groups, rows, start_ref, item_ref, before_ref, mine_ref, other_ref, *rest):
    n = len(groups)
    bufs, out_ref, own, acc = rest[:n], rest[n], rest[n + 1], rest[n + 2]
    held, sem, own_sem = rest[n + 3 : 2 * n + 3], rest[-2], rest[-1]
    half = mine_ref.shape[0]
    slots_here = half // rows
    first = pltpu.make_async_copy(mine_ref, own.at[pl.ds(0, half)], own_sem.at[0])
    second = pltpu.make_async_copy(other_ref, own.at[pl.ds(half, half)], own_sem.at[1])
    first.start()
    second.start()
    for i, group in enumerate(groups):

        @pl.when(start_ref[0, group + 1] > start_ref[0, group])
        def _(i=i):
            pltpu.make_async_copy(bufs[i], held[i], sem.at[i]).start()

    own[2 * half] = jnp.zeros(own.shape[1:], own.dtype)
    acc[...] = jnp.zeros_like(acc)
    first.wait()
    second.wait()

    def work(group, source):
        def step(i, carry):
            for u in range(UNROLL):
                n = i * UNROLL + u
                code = item_ref[n >> 7, n & 127]
                a = code & 255
                b = (code >> 8) & 255
                t = code >> 16
                row = (a & (half - 1)) // slots_here
                product = jnp.dot(own[a], source[t], preferred_element_type=jnp.float32)
                acc[row] += product * own[b].astype(jnp.float32)
            return carry

        lax.fori_loop(start_ref[0, group], start_ref[0, group + 1], step, 0)

    if not groups:
        work(OWN, own)
    for i, group in enumerate(groups):

        @pl.when(start_ref[0, group + 1] > start_ref[0, group])
        def _(i=i, group=group):
            pltpu.make_async_copy(bufs[i], held[i], sem.at[i]).wait()
            work(group, held[i])

    out_ref[...] = before_ref[...] + jnp.sum(acc[...], axis=2)


def count_tiles(groups, rows, starts, items, before, mine, other, bufs, flops):
    half, tile, _ = mine.shape
    anywhere = pl.BlockSpec(memory_space=pl.ANY)
    vmem = pl.BlockSpec(memory_space=pltpu.VMEM)
    return pl.pallas_call(
        lambda *refs: count_kernel(groups, rows, *refs),
        out_shape=jax.ShapeDtypeStruct((rows, tile), jnp.float32),
        in_specs=[pl.BlockSpec(memory_space=pltpu.SMEM)] * 2 + [vmem] + [anywhere] * (2 + len(bufs)),
        out_specs=vmem,
        scratch_shapes=[
            pltpu.VMEM((2 * half + 1, tile, tile), mine.dtype),
            pltpu.VMEM((rows, tile, tile), jnp.float32),
        ]
        + [pltpu.VMEM(b.shape, b.dtype) for b in bufs]
        + [pltpu.SemaphoreType.DMA((max(1, len(bufs)),)), pltpu.SemaphoreType.DMA((2,))],
        cost_estimate=pl.CostEstimate(flops=flops, bytes_accessed=8 * 10**6, transcendentals=0),
    )(starts, items, before, mine, other, *bufs)


def list_kernel(cut, half, near_ref, spot_ref, row_ref, column_ref, group_ref, a_ref, b_ref, start_ref, item_ref):
    slots, lanes = near_ref.shape
    f32, bf16 = jnp.float32, jnp.bfloat16
    down = lax.broadcasted_iota(jnp.int32, (lanes, lanes), 0)
    across = lax.broadcasted_iota(jnp.int32, (lanes, lanes), 1)

    where = jnp.zeros((lanes, lanes), jnp.int32)
    for s in range(slots):
        where = where + jnp.where(down == near_ref[s : s + 1], spot_ref[s : s + 1], 0)
    line = (down == row_ref[...]).astype(bf16)
    where = jnp.dot(where.astype(bf16), line, preferred_element_type=f32)
    column = (across == column_ref[...]).astype(bf16)
    found = jnp.dot(column, where.astype(bf16), preferred_element_type=f32)
    found = jnp.where(down // slots == across // slots, found, 0.0).astype(bf16)
    fold = lax.broadcasted_iota(jnp.int32, (slots, lanes), 0)
    fold = fold == lax.broadcasted_iota(jnp.int32, (slots, lanes), 1) % slots
    found = jnp.dot(fold.astype(bf16), found, preferred_element_type=f32).astype(jnp.int32)

    group = jnp.broadcast_to(group_ref[...], found.shape)
    for split in SPLIT:
        second = (group_ref[...] == split) & (found > cut)
        group = jnp.where(second, split + 1, group)
        found = jnp.where(second, found - cut, found)

    chosen = [((group == g) & (found > 0)).astype(f32) for g in range(GROUPS)]
    stack = jnp.concatenate(chosen, axis=0).astype(bf16)
    before = (down < across).astype(bf16)
    rank = jnp.dot(stack, before, preferred_element_type=f32)
    sums = jnp.dot(stack, jnp.ones((lanes, lanes), bf16), preferred_element_type=f32)
    above = lax.broadcasted_iota(jnp.int32, (slots, slots), 0)
    above = (above > lax.broadcasted_iota(jnp.int32, (slots, slots), 1)).astype(bf16)
    start = jnp.zeros((1, lanes), f32)
    target = jnp.zeros((slots, lanes), f32)
    starts = jnp.zeros(start_ref.shape, f32)
    lane = lax.broadcasted_iota(jnp.int32, start_ref.shape, 1)
    for g in range(GROUPS):
        part = slice(g * slots, (g + 1) * slots)
        ahead = jnp.dot(above, sums[part].astype(bf16), preferred_element_type=f32)
        place = rank[part] + ahead + start * UNROLL + 1.0
        target = target + chosen[g] * place
        trips = jnp.floor((jnp.sum(sums[part], axis=0, keepdims=True) + (UNROLL - 1)) / UNROLL)
        start = start + trips
        starts = jnp.where(lane == g + 1, start, starts)
    start_ref[...] = starts.astype(jnp.int32)

    high = lax.broadcasted_iota(jnp.int32, (item_ref.shape[0], lanes), 0)
    target = target.astype(jnp.int32) - 1
    total = jnp.zeros((3 * item_ref.shape[0], lanes), f32)
    for q in range(slots):
        t = target[q : q + 1]
        major, minor = t >> 7, t & 127
        fields = (a_ref[...], 2 * half - b_ref[q : q + 1], found[q : q + 1] - 1)
        left = [jnp.where(high == major, field, 0).astype(f32) for field in fields]
        left = jnp.concatenate(left, axis=0).astype(bf16)
        right = (down == minor).astype(bf16)
        total = total + lax.dot_general(
            left, right, (((1,), (1,)), ((), ())), preferred_element_type=f32
        )
    total = total.astype(jnp.int32)
    n = item_ref.shape[0]
    item_ref[...] = total[:n] + (2 * half - total[n : 2 * n]) * 256 + total[2 * n :] * 65536


def list_inputs(tile_cols, lists, ranks, rows, here, core, loc):
    _, slots = tile_cols.shape
    per_block = rows * slots
    window = (BACK + 1) * rows
    place = here % BACK

    pad = ((BACK, 0), (0, 0), (0, 0))
    near_lists = lax.dynamic_slice_in_dim(jnp.pad(lists, pad), here, BACK, 0)
    near_ranks = lax.dynamic_slice_in_dim(jnp.pad(ranks, pad), here, BACK, 0)
    from_place = (here + jnp.arange(BACK)) % BACK
    dist = BACK - jnp.arange(BACK)
    upper = (dist == 4) | ((dist == 1) & (from_place == 3))
    upper = upper | ((dist == 3) & ((from_place == 1) | (from_place == 2)))
    which = jnp.where(dist == 2, 1, jnp.where(upper, 2, 0))
    pick = (which[:, None] == jnp.arange(3))[:, :, None]
    flag = jnp.any(near_lists & pick, axis=1)
    rank = jnp.sum(jnp.where(pick, near_ranks, 0), axis=1)
    spot = jnp.where(flag & (rank % 2 == core), rank // 2 + 1, 0)
    order = jnp.arange(per_block, dtype=jnp.int32)
    own_spot = jnp.where(order % 2 == core, loc + 1, 0)
    spot = jnp.concatenate([spot, own_spot[None]], axis=0).reshape(window, slots)

    base = (here - BACK) * rows
    padded = jnp.pad(tile_cols, ((BACK * rows, 0), (0, 0)), constant_values=-1)
    near = lax.dynamic_slice(padded, (here * rows, 0), (window, slots))
    near = jnp.where(near >= 0, near - base, -1)
    mine = near[BACK * rows :]
    back = BACK - mine // rows
    group = jnp.zeros_like(back)
    for row in range(BACK):
        for d in range(1, BACK + 1):
            group = jnp.where((place == row) & (back == d), ARRIVES[row][d - 1], group)
    wide = ((0, 0), (0, per_block - window))
    return (
        jnp.pad(near.T, wide, constant_values=-1),
        jnp.pad(spot.T, wide),
        mine.reshape(1, per_block),
        mine.reshape(per_block, 1),
        group.reshape(1, per_block),
        loc.reshape(1, per_block),
        jnp.repeat(loc.reshape(rows, slots).T, slots, axis=1),
    )


def work_list(inputs, cut, rows, half):
    slots, lanes = inputs[0].shape
    limit = rows * slots * (slots + 1) // 2 + GROUPS * UNROLL
    depth = -(-limit // (8 * lanes)) * 8
    vmem = pl.BlockSpec(memory_space=pltpu.VMEM)
    return pl.pallas_call(
        lambda *refs: list_kernel(cut, half, *refs),
        out_shape=[
            jax.ShapeDtypeStruct((8, lanes), jnp.int32),
            jax.ShapeDtypeStruct((depth, lanes), jnp.int32),
        ],
        in_specs=[vmem] * len(inputs),
        out_specs=[vmem, vmem],
        cost_estimate=pl.CostEstimate(flops=10**9, bytes_accessed=10**5, transcendentals=0),
    )(*inputs)


def body(tiles, tile_cols):
    rows, half_slots, tile, _ = tiles.shape
    _, slots = tile_cols.shape
    core = lax.axis_index("rep")
    here = lax.axis_index("row")
    half = rows * half_slots
    per_block = rows * slots
    mine = tiles.reshape(half, tile, tile)
    other = swap_cores(mine)

    lists, ranks, ahead = send_lists(tile_cols, rows)
    totals = jnp.sum(lists.astype(jnp.int32), axis=2)
    slot = jnp.arange(per_block, dtype=jnp.int32)
    line, column = slot // slots, slot % slots
    loc = ((column // half_slots) ^ core) * half + line * half_slots + column % half_slots

    full = per_block // 2
    my_list = lax.dynamic_index_in_dim(lists, here, 0, False)
    my_rank = lax.dynamic_index_in_dim(ranks, here, 0, False)
    want = (jnp.arange(full, dtype=jnp.int32) * 2 + core)[None, :, None]
    match = my_list[:, None, :] & (my_rank[:, None, :] == want)
    index = jnp.sum(jnp.where(match, loc, 0), axis=2)

    def run(caps):
        cut, rest = caps[0], caps[1]

        def exchange(mine, other, index, inputs):
            pieces = [(0, 0, cut), (1, 0, caps[2]), (2, 0, caps[3]), (2, 0, caps[4])]
            pieces += [(0, cut, rest)] * (rest > 0)
            sent = gather_tiles(pieces, index, mine, other)
            sent, inputs = lax.optimization_barrier((sent, inputs))
            pair = {0: 1, 1: -1, 2: 1, 3: -1}
            side0 = moved(sent[0], pair)
            up3 = moved(sent[2], {3: 4})
            second = moved(sent[1], {0: 2, 1: 2, 2: -2, 3: -2})
            up = moved(sent[3], {0: 4, 1: 4, 2: 4})
            side1 = moved(sent[4], pair) if rest else None
            starts, items = work_list(inputs, cut, rows, half)
            counts = jnp.zeros((rows, tile), jnp.float32)
            counts = count_tiles((), rows, starts, items, counts, mine, other, [], 10**9)
            side0, counts = lax.optimization_barrier((side0, counts))
            side_next0 = moved(side0, {0: 2, 1: 2})
            side_up = moved(side0, {2: 4})
            up_down = moved(up, {1: -1, 2: -1})
            next_up = moved(second, {0: 4, 1: 4})
            up3_diag = moved(up3, {3: -3})
            early = {SIDE0: side0, NEXT: second, UP3: up3, UP: up}
            middle = {SIDE_NEXT0: side_next0, SIDE_UP: side_up, NEXT_UP: next_up, UP_DOWN: up_down}
            late = {UP3_DIAG: up3_diag}
            if rest:
                early[SIDE1] = side1
                late[SIDE_NEXT1] = moved(side1, {0: 2})
            for bufs in (early, middle, late):
                counts = count_tiles(
                    tuple(bufs), rows, starts, items, counts, mine, other, list(bufs.values()), 10**9
                )
            return counts

        return exchange

    place = jnp.arange(totals.shape[0]) % BACK

    def fit(caps):
        upper = jnp.where(place == 3, caps[3], caps[4])
        sizes = jnp.stack([ahead, totals[:, 0], totals[:, 1], totals[:, 2]], axis=1)
        bound = [jnp.full_like(place, c) for c in (caps[0], caps[0] + caps[1], caps[2])] + [upper]
        return jnp.all(sizes <= 2 * jnp.stack(bound, axis=1))

    brief = (full * 7 // 16, full * 5 // 16, full * 5 // 8, full * 11 // 16, full * 15 // 32)
    most = (full, 0, full, full, full)
    inputs = list_inputs(tile_cols, lists, ranks, rows, here, core, loc)
    partial = lax.cond(fit(brief), run(brief), run(most), mine, other, index, inputs)

    width = tile // 2
    keep = lax.dynamic_slice_in_dim(partial, core * width, width, 1)
    give = lax.dynamic_slice_in_dim(partial, (1 - core) * width, width, 1)
    return keep + swap_cores(give)


def solution(mesh):
    return jax.shard_map(
        body,
        mesh=mesh,
        in_specs=(P("row", "rep", None, None), P()),
        out_specs=P("row", "rep"),
        check_vma=False,
    )
```

```python
import jax
import jax.numpy as jnp
import numpy as np
from jax import lax
from jax.experimental import pallas as pl
from jax.experimental.pallas import tpu as pltpu
from jax.sharding import PartitionSpec as P


BACK = 4
UNROLL = 8
(OWN, SIDE0, SIDE1, NEXT, UP3A, UP3B, UP) = range(7)
(SIDE_NEXT0, SIDE_NEXT1, SIDE_UP, NEXT_UP, DIAGA, DIAGB, UP_DOWN) = range(7, 14)
GROUPS = 14
SPLIT = (SIDE0, SIDE_NEXT0, UP3A, DIAGA)
ARRIVES = (
    (DIAGA, NEXT_UP, UP_DOWN, UP),
    (SIDE0, NEXT_UP, UP_DOWN, UP),
    (SIDE_NEXT0, NEXT, SIDE_UP, UP),
    (SIDE0, NEXT, SIDE_NEXT0, UP3A),
)


def swap_cores(x):
    return lax.ppermute(x, "rep", [(0, 1), (1, 0)])


def moved(x, steps):
    size = lax.axis_size("row")
    route = [(i, i + steps[i % BACK]) for i in range(size) if i % BACK in steps]
    return lax.ppermute(x, "row", [(i, j) for i, j in route if j < size])


def running(flags):
    n = flags.shape[-1]
    tri = (jnp.arange(n)[:, None] < jnp.arange(n)[None, :]).astype(jnp.bfloat16)
    flat = flags.reshape(-1, n).astype(jnp.bfloat16)
    count = jnp.dot(flat, tri, preferred_element_type=jnp.float32)
    return count.astype(jnp.int32).reshape(flags.shape)


def send_lists(tile_cols, rows):
    count, slots = tile_cols.shape
    blocks = count // rows
    every = jnp.arange(count, dtype=jnp.int32)
    hot = tile_cols[:, :, None] == every
    member = jnp.any(hot, axis=1).astype(jnp.bfloat16).reshape(blocks, rows, count)
    padded = jnp.pad(member, ((0, BACK), (0, 0), (0, 0)))
    later = jnp.concatenate([padded[d : d + blocks] for d in range(1, BACK + 1)], axis=1)
    column = hot.reshape(blocks, rows * slots, count).astype(jnp.bfloat16)
    line = jnp.broadcast_to((every[:, None] == every)[:, None, :], hot.shape)
    line = line.reshape(blocks, rows * slots, count).astype(jnp.bfloat16)
    dims = (((2,), (2,)), ((0,), (0,)))
    has_column = lax.dot_general(later, column, dims, preferred_element_type=jnp.float32)
    has_line = lax.dot_general(later, line, dims, preferred_element_type=jnp.float32)
    both = (has_column * has_line).reshape(blocks, BACK, rows, rows * slots)
    need = jnp.max(both, axis=2) > 0
    place = (jnp.arange(blocks) % BACK)[:, None]
    near, second, third, fourth = (need[:, d] for d in range(BACK))
    side = (near & (place != 3)) | (third & ((place == 0) | (place == 3)))
    upper = fourth | (near & (place == 3)) | (third & ((place == 1) | (place == 2)))
    lists = jnp.stack([side, second, upper], axis=1)
    ahead = side & third & ((place == 0) | (place == 3))
    order = running(jnp.concatenate([lists, ahead[:, None]], axis=1))
    first = order[:, 3]
    total = jnp.sum(ahead.astype(jnp.int32), axis=1, keepdims=True)
    side_rank = jnp.where(ahead, first, order[:, 0] - first + total)
    ranks = jnp.concatenate([side_rank[:, None], order[:, 1:3]], axis=1)
    return lists, ranks, total[:, 0]


def gather_kernel(pieces, index_ref, mine_ref, other_ref, *rest):
    outs, pool, sem = rest[:-2], rest[-2], rest[-1]
    half = mine_ref.shape[0]
    first = pltpu.make_async_copy(mine_ref, pool.at[pl.ds(0, half)], sem.at[0])
    second = pltpu.make_async_copy(other_ref, pool.at[pl.ds(half, half)], sem.at[1])
    first.start()
    second.start()
    first.wait()
    second.wait()
    for out, (which, start, cap) in zip(outs, pieces):

        def one(p, carry, out=out, which=which, start=start):
            out[p] = pool[index_ref[which, start + p]]
            return carry

        lax.fori_loop(0, cap, one, 0, unroll=2)


def gather_tiles(pieces, index, mine, other):
    tile = mine.shape[-2:]
    anywhere = pl.BlockSpec(memory_space=pl.ANY)
    total = sum(cap for _, _, cap in pieces)
    return pl.pallas_call(
        lambda *refs: gather_kernel(pieces, *refs),
        out_shape=[jax.ShapeDtypeStruct((cap,) + tile, mine.dtype) for _, _, cap in pieces],
        in_specs=[pl.BlockSpec(memory_space=pltpu.SMEM), anywhere, anywhere],
        out_specs=[pl.BlockSpec(memory_space=pltpu.VMEM)] * len(pieces),
        scratch_shapes=[
            pltpu.VMEM((2 * mine.shape[0],) + tile, mine.dtype),
            pltpu.SemaphoreType.DMA((2,)),
        ],
        cost_estimate=pl.CostEstimate(
            flops=10**6, bytes_accessed=total * 65536, transcendentals=0
        ),
    )(index, mine, other)


def count_kernel(groups, rows, start_ref, item_ref, before_ref, mine_ref, other_ref, *rest):
    n = len(groups)
    bufs, out_ref, own, acc = rest[:n], rest[n], rest[n + 1], rest[n + 2]
    held, sem, own_sem = rest[n + 3 : 2 * n + 3], rest[-2], rest[-1]
    half = mine_ref.shape[0]
    slots_here = half // rows
    first = pltpu.make_async_copy(mine_ref, own.at[pl.ds(0, half)], own_sem.at[0])
    second = pltpu.make_async_copy(other_ref, own.at[pl.ds(half, half)], own_sem.at[1])
    first.start()
    second.start()
    for i, group in enumerate(groups):

        @pl.when(start_ref[0, group + 1] > start_ref[0, group])
        def _(i=i):
            pltpu.make_async_copy(bufs[i], held[i], sem.at[i]).start()

    own[2 * half] = jnp.zeros(own.shape[1:], own.dtype)
    acc[...] = jnp.zeros_like(acc)
    first.wait()
    second.wait()

    def work(group, source):
        def step(i, carry):
            for u in range(UNROLL):
                n = i * UNROLL + u
                code = item_ref[n >> 7, n & 127]
                a = code & 255
                b = (code >> 8) & 255
                t = code >> 16
                row = (a & (half - 1)) // slots_here
                product = jnp.dot(own[a], source[t], preferred_element_type=jnp.float32)
                acc[row] += product * own[b].astype(jnp.float32)
            return carry

        lax.fori_loop(start_ref[0, group], start_ref[0, group + 1], step, 0)

    if not groups:
        work(OWN, own)
    for i, group in enumerate(groups):

        @pl.when(start_ref[0, group + 1] > start_ref[0, group])
        def _(i=i, group=group):
            pltpu.make_async_copy(bufs[i], held[i], sem.at[i]).wait()
            work(group, held[i])

    out_ref[...] = before_ref[...] + jnp.sum(acc[...], axis=2)


def count_tiles(groups, rows, starts, items, before, mine, other, bufs, flops):
    half, tile, _ = mine.shape
    anywhere = pl.BlockSpec(memory_space=pl.ANY)
    vmem = pl.BlockSpec(memory_space=pltpu.VMEM)
    return pl.pallas_call(
        lambda *refs: count_kernel(groups, rows, *refs),
        out_shape=jax.ShapeDtypeStruct((rows, tile), jnp.float32),
        in_specs=[pl.BlockSpec(memory_space=pltpu.SMEM)] * 2 + [vmem] + [anywhere] * (2 + len(bufs)),
        out_specs=vmem,
        scratch_shapes=[
            pltpu.VMEM((2 * half + 1, tile, tile), mine.dtype),
            pltpu.VMEM((rows, tile, tile), jnp.float32),
        ]
        + [pltpu.VMEM(b.shape, b.dtype) for b in bufs]
        + [pltpu.SemaphoreType.DMA((max(1, len(bufs)),)), pltpu.SemaphoreType.DMA((2,))],
        cost_estimate=pl.CostEstimate(flops=flops, bytes_accessed=8 * 10**6, transcendentals=0),
    )(starts, items, before, mine, other, *bufs)


def list_kernel(cuts, half, near_ref, spot_ref, row_ref, column_ref, group_ref, a_ref, b_ref, start_ref, item_ref):
    slots, lanes = near_ref.shape
    f32, bf16 = jnp.float32, jnp.bfloat16
    down = lax.broadcasted_iota(jnp.int32, (lanes, lanes), 0)
    across = lax.broadcasted_iota(jnp.int32, (lanes, lanes), 1)

    where = jnp.zeros((lanes, lanes), jnp.int32)
    for s in range(slots):
        where = where + jnp.where(down == near_ref[s : s + 1], spot_ref[s : s + 1], 0)
    line = (down == row_ref[...]).astype(bf16)
    where = jnp.dot(where.astype(bf16), line, preferred_element_type=f32)
    column = (across == column_ref[...]).astype(bf16)
    found = jnp.dot(column, where.astype(bf16), preferred_element_type=f32)
    found = jnp.where(down // slots == across // slots, found, 0.0).astype(bf16)
    fold = lax.broadcasted_iota(jnp.int32, (slots, lanes), 0)
    fold = fold == lax.broadcasted_iota(jnp.int32, (slots, lanes), 1) % slots
    found = jnp.dot(fold.astype(bf16), found, preferred_element_type=f32).astype(jnp.int32)

    group = jnp.broadcast_to(group_ref[...], found.shape)
    for split in SPLIT:
        cut = cuts[split in (UP3A, DIAGA)]
        second = (group_ref[...] == split) & (found > cut)
        group = jnp.where(second, split + 1, group)
        found = jnp.where(second, found - cut, found)

    chosen = [((group == g) & (found > 0)).astype(f32) for g in range(GROUPS)]
    stack = jnp.concatenate(chosen, axis=0).astype(bf16)
    before = (down < across).astype(bf16)
    rank = jnp.dot(stack, before, preferred_element_type=f32)
    sums = jnp.dot(stack, jnp.ones((lanes, lanes), bf16), preferred_element_type=f32)
    above = lax.broadcasted_iota(jnp.int32, (slots, slots), 0)
    above = (above > lax.broadcasted_iota(jnp.int32, (slots, slots), 1)).astype(bf16)
    start = jnp.zeros((1, lanes), f32)
    target = jnp.zeros((slots, lanes), f32)
    starts = jnp.zeros(start_ref.shape, f32)
    lane = lax.broadcasted_iota(jnp.int32, start_ref.shape, 1)
    for g in range(GROUPS):
        part = slice(g * slots, (g + 1) * slots)
        ahead = jnp.dot(above, sums[part].astype(bf16), preferred_element_type=f32)
        place = rank[part] + ahead + start * UNROLL + 1.0
        target = target + chosen[g] * place
        trips = jnp.floor((jnp.sum(sums[part], axis=0, keepdims=True) + (UNROLL - 1)) / UNROLL)
        start = start + trips
        starts = jnp.where(lane == g + 1, start, starts)
    start_ref[...] = starts.astype(jnp.int32)

    high = lax.broadcasted_iota(jnp.int32, (item_ref.shape[0], lanes), 0)
    target = target.astype(jnp.int32) - 1
    total = jnp.zeros((3 * item_ref.shape[0], lanes), f32)
    for q in range(slots):
        t = target[q : q + 1]
        major, minor = t >> 7, t & 127
        fields = (a_ref[...], 2 * half - b_ref[q : q + 1], found[q : q + 1] - 1)
        left = [jnp.where(high == major, field, 0).astype(f32) for field in fields]
        left = jnp.concatenate(left, axis=0).astype(bf16)
        right = (down == minor).astype(bf16)
        total = total + lax.dot_general(
            left, right, (((1,), (1,)), ((), ())), preferred_element_type=f32
        )
    total = total.astype(jnp.int32)
    n = item_ref.shape[0]
    item_ref[...] = total[:n] + (2 * half - total[n : 2 * n]) * 256 + total[2 * n :] * 65536


def list_inputs(tile_cols, lists, ranks, rows, here, core, loc):
    _, slots = tile_cols.shape
    per_block = rows * slots
    window = (BACK + 1) * rows
    place = here % BACK

    pad = ((BACK, 0), (0, 0), (0, 0))
    near_lists = lax.dynamic_slice_in_dim(jnp.pad(lists, pad), here, BACK, 0)
    near_ranks = lax.dynamic_slice_in_dim(jnp.pad(ranks, pad), here, BACK, 0)
    from_place = (here + jnp.arange(BACK)) % BACK
    dist = BACK - jnp.arange(BACK)
    upper = (dist == 4) | ((dist == 1) & (from_place == 3))
    upper = upper | ((dist == 3) & ((from_place == 1) | (from_place == 2)))
    which = jnp.where(dist == 2, 1, jnp.where(upper, 2, 0))
    pick = (which[:, None] == jnp.arange(3))[:, :, None]
    flag = jnp.any(near_lists & pick, axis=1)
    rank = jnp.sum(jnp.where(pick, near_ranks, 0), axis=1)
    spot = jnp.where(flag & (rank % 2 == core), rank // 2 + 1, 0)
    order = jnp.arange(per_block, dtype=jnp.int32)
    own_spot = jnp.where(order % 2 == core, loc + 1, 0)
    spot = jnp.concatenate([spot, own_spot[None]], axis=0).reshape(window, slots)

    base = (here - BACK) * rows
    padded = jnp.pad(tile_cols, ((BACK * rows, 0), (0, 0)), constant_values=-1)
    near = lax.dynamic_slice(padded, (here * rows, 0), (window, slots))
    near = jnp.where(near >= 0, near - base, -1)
    mine = near[BACK * rows :]
    back = BACK - mine // rows
    group = jnp.zeros_like(back)
    for row in range(BACK):
        for d in range(1, BACK + 1):
            group = jnp.where((place == row) & (back == d), ARRIVES[row][d - 1], group)
    wide = ((0, 0), (0, per_block - window))
    return (
        jnp.pad(near.T, wide, constant_values=-1),
        jnp.pad(spot.T, wide),
        mine.reshape(1, per_block),
        mine.reshape(per_block, 1),
        group.reshape(1, per_block),
        loc.reshape(1, per_block),
        jnp.repeat(loc.reshape(rows, slots).T, slots, axis=1),
    )


def work_list(inputs, cuts, rows, half):
    slots, lanes = inputs[0].shape
    limit = rows * slots * (slots + 1) // 2 + GROUPS * UNROLL
    depth = -(-limit // (8 * lanes)) * 8
    vmem = pl.BlockSpec(memory_space=pltpu.VMEM)
    return pl.pallas_call(
        lambda *refs: list_kernel(cuts, half, *refs),
        out_shape=[
            jax.ShapeDtypeStruct((8, lanes), jnp.int32),
            jax.ShapeDtypeStruct((depth, lanes), jnp.int32),
        ],
        in_specs=[vmem] * len(inputs),
        out_specs=[vmem, vmem],
        cost_estimate=pl.CostEstimate(flops=10**9, bytes_accessed=10**5, transcendentals=0),
    )(*inputs)


def body(tiles, tile_cols):
    rows, half_slots, tile, _ = tiles.shape
    _, slots = tile_cols.shape
    core = lax.axis_index("rep")
    here = lax.axis_index("row")
    half = rows * half_slots
    per_block = rows * slots
    mine = tiles.reshape(half, tile, tile)
    other = swap_cores(mine)

    lists, ranks, ahead = send_lists(tile_cols, rows)
    totals = jnp.sum(lists.astype(jnp.int32), axis=2)
    slot = jnp.arange(per_block, dtype=jnp.int32)
    line, column = slot // slots, slot % slots
    loc = ((column // half_slots) ^ core) * half + line * half_slots + column % half_slots

    full = per_block // 2
    my_list = lax.dynamic_index_in_dim(lists, here, 0, False)
    my_rank = lax.dynamic_index_in_dim(ranks, here, 0, False)
    want = (jnp.arange(full, dtype=jnp.int32) * 2 + core)[None, :, None]
    match = my_list[:, None, :] & (my_rank[:, None, :] == want)
    index = jnp.sum(jnp.where(match, loc, 0), axis=2)

    def run(caps):
        (side_a, side_b), next_cap, (up3_a, up3_b), up_cap = caps

        def exchange(mine, other, index, inputs):
            pieces = [(0, 0, side_a), (2, 0, up3_a), (1, 0, next_cap)]
            pieces += [(0, side_a, side_b), (2, up3_a, up3_b)] * (side_b > 0)
            pieces += [(2, 0, up_cap)]
            sent = gather_tiles(pieces, index, mine, other)
            sent, group = lax.optimization_barrier((sent, inputs[4]))
            inputs = inputs[:4] + (group,) + inputs[5:]
            early, middle, late = {}, {}, {}
            early[SIDE0] = side0 = moved(sent[0], {0: 1, 1: -1, 2: 1, 3: -1})
            early[UP3A] = moved(sent[1], {3: 4})
            early[NEXT] = moved(sent[2], {0: 2, 1: 2, 2: -2, 3: -2})
            if side_b:
                early[SIDE1] = moved(sent[3], {0: 1, 1: -1, 2: 1})
                early[UP3B] = moved(sent[4], {3: 4})
            early[UP] = moved(sent[-1], {0: 4, 1: 4, 2: 4})
            starts, items = work_list(inputs, (side_a, up3_a), rows, half)
            counts = jnp.zeros((rows, tile), jnp.float32)
            counts = count_tiles((), rows, starts, items, counts, mine, other, [], 10**9)
            second, counts = lax.optimization_barrier((early[NEXT], counts))
            middle[SIDE_NEXT0] = moved(side0, {0: 2, 1: 2})
            middle[SIDE_UP] = moved(side0, {2: 4})
            middle[DIAGA] = moved(early[UP3A], {3: -3})
            late[UP_DOWN] = moved(early[UP], {1: -1, 2: -1})
            middle[NEXT_UP] = moved(second, {0: 4, 1: 4})
            if side_b:
                late[DIAGB] = moved(early[UP3B], {3: -3})
                late[SIDE_NEXT1] = moved(early[SIDE1], {0: 2})
            for bufs in (early, middle, late):
                counts = count_tiles(
                    tuple(bufs), rows, starts, items, counts, mine, other, list(bufs.values()), 10**9
                )
            return counts

        return exchange

    unit = full // 32
    tiers = (
        ((12 * unit, 12 * unit), 17 * unit, (11 * unit, 10 * unit), 13 * unit),
        ((13 * unit, 12 * unit), 19 * unit, (12 * unit, 10 * unit), 15 * unit),
        ((14 * unit, 14 * unit), 23 * unit, (13 * unit, 12 * unit), 20 * unit),
        ((full, 0), full, (full, 0), full),
    )
    bounds = np.zeros((len(tiers) - 1, BACK, 4), np.int32)
    for bound, (side, second, up3, up) in zip(bounds, tiers):
        for at in range(BACK):
            upper = sum(up3) if at == BACK - 1 else up
            bound[at] = (2 * side[0], 2 * sum(side), 2 * second, 2 * upper)
    sizes = jnp.concatenate([ahead[:, None], totals], axis=1).reshape(1, -1, BACK, 4)
    fits = jnp.all(sizes <= bounds[:, None], axis=(1, 2, 3))
    choice = len(tiers) - 1 - jnp.sum(fits.astype(jnp.int32))
    inputs = list_inputs(tile_cols, lists, ranks, rows, here, core, loc)
    runs = [run(caps) for caps in tiers]
    partial = lax.switch(choice, runs, mine, other, index, inputs)

    width = tile // 2
    keep = lax.dynamic_slice_in_dim(partial, core * width, width, 1)
    give = lax.dynamic_slice_in_dim(partial, (1 - core) * width, width, 1)
    return keep + swap_cores(give)


def solution(mesh):
    return jax.shard_map(
        body,
        mesh=mesh,
        in_specs=(P("row", "rep", None, None), P()),
        out_specs=P("row", "rep"),
        check_vma=False,
    )
```

```python
import jax
import jax.numpy as jnp
import numpy as np
from jax import lax
from jax.experimental import pallas as pl
from jax.experimental.pallas import tpu as pltpu
from jax.sharding import PartitionSpec as P


BACK = 4
UNROLL = 8
(OWN, SIDE0, SIDE1, NEXT, UP3A, UP3B, UP) = range(7)
(SIDE_NEXT0, SIDE_NEXT1, SIDE_UP, NEXT_UP, DIAGA, DIAGB, UP_DOWN) = range(7, 14)
GROUPS = 14
SPLIT = (SIDE0, SIDE_NEXT0, UP3A, DIAGA)
ARRIVES = (
    (DIAGA, NEXT_UP, UP_DOWN, UP),
    (SIDE0, NEXT_UP, UP_DOWN, UP),
    (SIDE_NEXT0, NEXT, SIDE_UP, UP),
    (SIDE0, NEXT, SIDE_NEXT0, UP3A),
)


def swap_cores(x):
    return lax.ppermute(x, "rep", [(0, 1), (1, 0)])


def moved(x, steps):
    size = lax.axis_size("row")
    route = [(i, i + steps[i % BACK]) for i in range(size) if i % BACK in steps]
    return lax.ppermute(x, "row", [(i, j) for i, j in route if j < size])


def running(flags):
    n = flags.shape[-1]
    tri = (jnp.arange(n)[:, None] < jnp.arange(n)[None, :]).astype(jnp.bfloat16)
    flat = flags.reshape(-1, n).astype(jnp.bfloat16)
    count = jnp.dot(flat, tri, preferred_element_type=jnp.float32)
    return count.astype(jnp.int32).reshape(flags.shape)


def send_lists(tile_cols, rows):
    count, slots = tile_cols.shape
    blocks = count // rows
    every = jnp.arange(count, dtype=jnp.int32)
    hot = tile_cols[:, :, None] == every
    member = jnp.any(hot, axis=1).astype(jnp.bfloat16).reshape(blocks, rows, count)
    padded = jnp.pad(member, ((0, BACK), (0, 0), (0, 0)))
    later = jnp.concatenate([padded[d : d + blocks] for d in range(1, BACK + 1)], axis=1)
    column = hot.reshape(blocks, rows * slots, count).astype(jnp.bfloat16)
    line = jnp.broadcast_to((every[:, None] == every)[:, None, :], hot.shape)
    line = line.reshape(blocks, rows * slots, count).astype(jnp.bfloat16)
    dims = (((2,), (2,)), ((0,), (0,)))
    has_column = lax.dot_general(later, column, dims, preferred_element_type=jnp.float32)
    has_line = lax.dot_general(later, line, dims, preferred_element_type=jnp.float32)
    both = (has_column * has_line).reshape(blocks, BACK, rows, rows * slots)
    need = jnp.max(both, axis=2) > 0
    place = (jnp.arange(blocks) % BACK)[:, None]
    near, second, third, fourth = (need[:, d] for d in range(BACK))
    side = (near & (place != 3)) | (third & ((place == 0) | (place == 3)))
    upper = fourth | (near & (place == 3)) | (third & ((place == 1) | (place == 2)))
    lists = jnp.stack([side, second, upper], axis=1)
    ahead = side & third & ((place == 0) | (place == 3))
    order = running(jnp.concatenate([lists, ahead[:, None]], axis=1))
    first = order[:, 3]
    total = jnp.sum(ahead.astype(jnp.int32), axis=1, keepdims=True)
    side_rank = jnp.where(ahead, first, order[:, 0] - first + total)
    ranks = jnp.concatenate([side_rank[:, None], order[:, 1:3]], axis=1)
    return lists, ranks, total[:, 0]


def gather_kernel(pieces, index_ref, mine_ref, other_ref, *rest):
    outs, pool, sem = rest[:-2], rest[-2], rest[-1]
    half = mine_ref.shape[0]
    first = pltpu.make_async_copy(mine_ref, pool.at[pl.ds(0, half)], sem.at[0])
    second = pltpu.make_async_copy(other_ref, pool.at[pl.ds(half, half)], sem.at[1])
    first.start()
    second.start()
    first.wait()
    second.wait()
    for out, (which, start, cap) in zip(outs, pieces):

        def one(p, carry, out=out, which=which, start=start):
            out[p] = pool[index_ref[which, start + p]]
            return carry

        lax.fori_loop(0, cap, one, 0, unroll=4)


def gather_tiles(pieces, index, mine, other):
    tile = mine.shape[-2:]
    anywhere = pl.BlockSpec(memory_space=pl.ANY)
    total = sum(cap for _, _, cap in pieces)
    return pl.pallas_call(
        lambda *refs: gather_kernel(pieces, *refs),
        out_shape=[jax.ShapeDtypeStruct((cap,) + tile, mine.dtype) for _, _, cap in pieces],
        in_specs=[pl.BlockSpec(memory_space=pltpu.SMEM), anywhere, anywhere],
        out_specs=[pl.BlockSpec(memory_space=pltpu.VMEM)] * len(pieces),
        scratch_shapes=[
            pltpu.VMEM((2 * mine.shape[0],) + tile, mine.dtype),
            pltpu.SemaphoreType.DMA((2,)),
        ],
        cost_estimate=pl.CostEstimate(
            flops=10**6, bytes_accessed=total * 65536, transcendentals=0
        ),
    )(index, mine, other)


def count_kernel(groups, rows, start_ref, item_ref, before_ref, mine_ref, other_ref, *rest):
    n = len(groups)
    bufs, out_ref, own, acc = rest[:n], rest[n], rest[n + 1], rest[n + 2]
    held, sem, own_sem = rest[n + 3 : 2 * n + 3], rest[-2], rest[-1]
    half = mine_ref.shape[0]
    slots_here = half // rows
    first = pltpu.make_async_copy(mine_ref, own.at[pl.ds(0, half)], own_sem.at[0])
    second = pltpu.make_async_copy(other_ref, own.at[pl.ds(half, half)], own_sem.at[1])
    first.start()
    second.start()
    for i, group in enumerate(groups):

        @pl.when(start_ref[0, group + 1] > start_ref[0, group])
        def _(i=i):
            pltpu.make_async_copy(bufs[i], held[i], sem.at[i]).start()

    own[2 * half] = jnp.zeros(own.shape[1:], own.dtype)
    acc[...] = jnp.zeros_like(acc)
    first.wait()
    second.wait()

    def work(group, source):
        def step(i, carry):
            for u in range(UNROLL):
                n = i * UNROLL + u
                code = item_ref[n >> 7, n & 127]
                a = code & 255
                b = (code >> 8) & 255
                t = code >> 16
                row = (a & (half - 1)) // slots_here
                product = jnp.dot(own[a], source[t], preferred_element_type=jnp.float32)
                acc[row] += product * own[b].astype(jnp.float32)
            return carry

        lax.fori_loop(start_ref[0, group], start_ref[0, group + 1], step, 0)

    if not groups:
        work(OWN, own)
    for i, group in enumerate(groups):

        @pl.when(start_ref[0, group + 1] > start_ref[0, group])
        def _(i=i, group=group):
            pltpu.make_async_copy(bufs[i], held[i], sem.at[i]).wait()
            work(group, held[i])

    out_ref[...] = before_ref[...] + jnp.sum(acc[...], axis=2)


def count_tiles(groups, rows, starts, items, before, mine, other, bufs, flops):
    half, tile, _ = mine.shape
    anywhere = pl.BlockSpec(memory_space=pltpu.HBM)
    vmem = pl.BlockSpec(memory_space=pltpu.VMEM)
    return pl.pallas_call(
        lambda *refs: count_kernel(groups, rows, *refs),
        out_shape=jax.ShapeDtypeStruct((rows, tile), jnp.float32),
        in_specs=[pl.BlockSpec(memory_space=pltpu.SMEM)] * 2 + [vmem] + [anywhere] * (2 + len(bufs)),
        out_specs=vmem,
        scratch_shapes=[
            pltpu.VMEM((2 * half + 1, tile, tile), mine.dtype),
            pltpu.VMEM((rows, tile, tile), jnp.float32),
        ]
        + [pltpu.VMEM(b.shape, b.dtype) for b in bufs]
        + [pltpu.SemaphoreType.DMA((max(1, len(bufs)),)), pltpu.SemaphoreType.DMA((2,))],
        cost_estimate=pl.CostEstimate(flops=flops, bytes_accessed=8 * 10**6, transcendentals=0),
    )(starts, items, before, mine, other, *bufs)


def list_kernel(cuts, half, near_ref, spot_ref, row_ref, column_ref, group_ref, a_ref, b_ref, start_ref, item_ref):
    slots, lanes = near_ref.shape
    f32, bf16 = jnp.float32, jnp.bfloat16
    down = lax.broadcasted_iota(jnp.int32, (lanes, lanes), 0)
    across = lax.broadcasted_iota(jnp.int32, (lanes, lanes), 1)

    where = jnp.zeros((lanes, lanes), jnp.int32)
    for s in range(slots):
        where = where + jnp.where(down == near_ref[s : s + 1], spot_ref[s : s + 1], 0)
    line = (down == row_ref[...]).astype(bf16)
    where = jnp.dot(where.astype(bf16), line, preferred_element_type=f32)
    column = (across == column_ref[...]).astype(bf16)
    found = jnp.dot(column, where.astype(bf16), preferred_element_type=f32)
    found = jnp.where(down // slots == across // slots, found, 0.0).astype(bf16)
    fold = lax.broadcasted_iota(jnp.int32, (slots, lanes), 0)
    fold = fold == lax.broadcasted_iota(jnp.int32, (slots, lanes), 1) % slots
    found = jnp.dot(fold.astype(bf16), found, preferred_element_type=f32).astype(jnp.int32)

    group = jnp.broadcast_to(group_ref[...], found.shape)
    for split in SPLIT:
        cut = cuts[split in (UP3A, DIAGA)]
        second = (group_ref[...] == split) & (found > cut)
        group = jnp.where(second, split + 1, group)
        found = jnp.where(second, found - cut, found)

    chosen = [((group == g) & (found > 0)).astype(f32) for g in range(GROUPS)]
    stack = jnp.concatenate(chosen, axis=0).astype(bf16)
    before = (down < across).astype(bf16)
    rank = jnp.dot(stack, before, preferred_element_type=f32)
    sums = jnp.dot(stack, jnp.ones((lanes, lanes), bf16), preferred_element_type=f32)
    above = lax.broadcasted_iota(jnp.int32, (slots, slots), 0)
    above = (above > lax.broadcasted_iota(jnp.int32, (slots, slots), 1)).astype(bf16)
    start = jnp.zeros((1, lanes), f32)
    target = jnp.zeros((slots, lanes), f32)
    starts = jnp.zeros(start_ref.shape, f32)
    lane = lax.broadcasted_iota(jnp.int32, start_ref.shape, 1)
    for g in range(GROUPS):
        part = slice(g * slots, (g + 1) * slots)
        ahead = jnp.dot(above, sums[part].astype(bf16), preferred_element_type=f32)
        place = rank[part] + ahead + start * UNROLL + 1.0
        target = target + chosen[g] * place
        trips = jnp.floor((jnp.sum(sums[part], axis=0, keepdims=True) + (UNROLL - 1)) / UNROLL)
        start = start + trips
        starts = jnp.where(lane == g + 1, start, starts)
    start_ref[...] = starts.astype(jnp.int32)

    high = lax.broadcasted_iota(jnp.int32, (item_ref.shape[0], lanes), 0)
    target = target.astype(jnp.int32) - 1
    total = jnp.zeros((3 * item_ref.shape[0], lanes), f32)
    for q in range(slots):
        t = target[q : q + 1]
        major, minor = t >> 7, t & 127
        fields = (a_ref[...], 2 * half - b_ref[q : q + 1], found[q : q + 1] - 1)
        left = [jnp.where(high == major, field, 0).astype(f32) for field in fields]
        left = jnp.concatenate(left, axis=0).astype(bf16)
        right = (down == minor).astype(bf16)
        total = total + lax.dot_general(
            left, right, (((1,), (1,)), ((), ())), preferred_element_type=f32
        )
    total = total.astype(jnp.int32)
    n = item_ref.shape[0]
    item_ref[...] = total[:n] + (2 * half - total[n : 2 * n]) * 256 + total[2 * n :] * 65536


def list_inputs(tile_cols, lists, ranks, rows, here, core, loc):
    _, slots = tile_cols.shape
    per_block = rows * slots
    window = (BACK + 1) * rows
    place = here % BACK

    pad = ((BACK, 0), (0, 0), (0, 0))
    near_lists = lax.dynamic_slice_in_dim(jnp.pad(lists, pad), here, BACK, 0)
    near_ranks = lax.dynamic_slice_in_dim(jnp.pad(ranks, pad), here, BACK, 0)
    from_place = (here + jnp.arange(BACK)) % BACK
    dist = BACK - jnp.arange(BACK)
    upper = (dist == 4) | ((dist == 1) & (from_place == 3))
    upper = upper | ((dist == 3) & ((from_place == 1) | (from_place == 2)))
    which = jnp.where(dist == 2, 1, jnp.where(upper, 2, 0))
    pick = (which[:, None] == jnp.arange(3))[:, :, None]
    flag = jnp.any(near_lists & pick, axis=1)
    rank = jnp.sum(jnp.where(pick, near_ranks, 0), axis=1)
    spot = jnp.where(flag & (rank % 2 == core), rank // 2 + 1, 0)
    order = jnp.arange(per_block, dtype=jnp.int32)
    own_spot = jnp.where(order % 2 == core, loc + 1, 0)
    spot = jnp.concatenate([spot, own_spot[None]], axis=0).reshape(window, slots)

    base = (here - BACK) * rows
    padded = jnp.pad(tile_cols, ((BACK * rows, 0), (0, 0)), constant_values=-1)
    near = lax.dynamic_slice(padded, (here * rows, 0), (window, slots))
    near = jnp.where(near >= 0, near - base, -1)
    mine = near[BACK * rows :]
    back = BACK - mine // rows
    group = jnp.zeros_like(back)
    for row in range(BACK):
        for d in range(1, BACK + 1):
            group = jnp.where((place == row) & (back == d), ARRIVES[row][d - 1], group)
    wide = ((0, 0), (0, per_block - window))
    return (
        jnp.pad(near.T, wide, constant_values=-1),
        jnp.pad(spot.T, wide),
        mine.reshape(1, per_block),
        mine.reshape(per_block, 1),
        group.reshape(1, per_block),
        loc.reshape(1, per_block),
        jnp.repeat(loc.reshape(rows, slots).T, slots, axis=1),
    )


def work_list(inputs, cuts, rows, half):
    slots, lanes = inputs[0].shape
    limit = rows * slots * (slots + 1) // 2 + GROUPS * UNROLL
    depth = -(-limit // (8 * lanes)) * 8
    vmem = pl.BlockSpec(memory_space=pltpu.VMEM)
    return pl.pallas_call(
        lambda *refs: list_kernel(cuts, half, *refs),
        out_shape=[
            jax.ShapeDtypeStruct((8, lanes), jnp.int32),
            jax.ShapeDtypeStruct((depth, lanes), jnp.int32),
        ],
        in_specs=[vmem] * len(inputs),
        out_specs=[vmem, vmem],
        cost_estimate=pl.CostEstimate(flops=10**9, bytes_accessed=10**5, transcendentals=0),
    )(*inputs)


def body(tiles, tile_cols):
    rows, half_slots, tile, _ = tiles.shape
    count, slots = tile_cols.shape
    core = lax.axis_index("rep")
    here = lax.axis_index("row")
    half = rows * half_slots
    per_block = rows * slots
    mine = tiles.reshape(half, tile, tile)
    other = swap_cores(mine)

    lists, ranks, ahead = send_lists(tile_cols, rows)
    totals = jnp.sum(lists.astype(jnp.int32), axis=2)
    slot = jnp.arange(per_block, dtype=jnp.int32)
    line, column = slot // slots, slot % slots
    loc = ((column // half_slots) ^ core) * half + line * half_slots + column % half_slots

    full = per_block // 2
    my_list = lax.dynamic_index_in_dim(lists, here, 0, False)
    my_rank = lax.dynamic_index_in_dim(ranks, here, 0, False)
    want = (jnp.arange(full, dtype=jnp.int32) * 2 + core)[None, :, None]
    match = my_list[:, None, :] & (my_rank[:, None, :] == want)
    index = jnp.sum(jnp.where(match, loc, 0), axis=2)

    def run(caps):
        (side_a, side_b), next_cap, (up3_a, up3_b), up_cap = caps

        def exchange(mine, other, index, inputs):
            pieces = [(0, 0, side_a), (2, 0, up3_a), (1, 0, next_cap)]
            pieces += [(0, side_a, side_b), (2, up3_a, up3_b)] * (side_b > 0)
            pieces += [(2, 0, up_cap)]
            sent = gather_tiles(pieces, index, mine, other)
            sent, group = lax.optimization_barrier((sent, inputs[4]))
            inputs = inputs[:4] + (group,) + inputs[5:]
            early, middle, late = {}, {}, {}
            early[SIDE0] = side0 = moved(sent[0], {0: 1, 1: -1, 2: 1, 3: -1})
            early[UP3A] = moved(sent[1], {3: 4})
            early[NEXT] = moved(sent[2], {0: 2, 1: 2, 2: -2, 3: -2})
            if side_b:
                early[SIDE1] = moved(sent[3], {0: 1, 1: -1, 2: 1})
                early[UP3B] = moved(sent[4], {3: 4})
            early[UP] = moved(sent[-1], {0: 4, 1: 4, 2: 4})
            starts, items = work_list(inputs, (side_a, up3_a), rows, half)
            counts = jnp.zeros((rows, tile), jnp.float32)
            counts = count_tiles((), rows, starts, items, counts, mine, other, [], 10**9)
            second, counts = lax.optimization_barrier((early[NEXT], counts))
            middle[SIDE_NEXT0] = moved(side0, {0: 2, 1: 2})
            middle[SIDE_UP] = moved(side0, {2: 4})
            middle[DIAGA] = moved(early[UP3A], {3: -3})
            middle[UP_DOWN] = moved(early[UP], {1: -1, 2: -1})
            middle[NEXT_UP] = moved(second, {0: 4, 1: 4})
            if side_b:
                late[DIAGB] = moved(early[UP3B], {3: -3})
                late[SIDE_NEXT1] = moved(early[SIDE1], {0: 2})
            for bufs in (early, middle, late):
                counts = count_tiles(
                    tuple(bufs), rows, starts, items, counts, mine, other, list(bufs.values()), 10**9
                )
            return counts

        return exchange

    unit = full // 32
    tiers = (
        ((12 * unit, 12 * unit), 17 * unit, (11 * unit, 10 * unit), 13 * unit),
        ((13 * unit, 12 * unit), 19 * unit, (12 * unit, 10 * unit), 15 * unit),
        ((14 * unit, 14 * unit), 23 * unit, (13 * unit, 12 * unit), 20 * unit),
        ((full, 0), full, (full, 0), full),
    )
    bounds = np.zeros((len(tiers) - 1, BACK, 4), np.int32)
    for bound, (side, second, up3, up) in zip(bounds, tiers):
        for at in range(BACK):
            upper = sum(up3) if at == BACK - 1 else up
            bound[at] = (2 * side[0], 2 * sum(side), 2 * second, 2 * upper)
    bounds = np.tile(bounds, (1, count // rows // BACK, 1))
    sizes = jnp.concatenate([ahead[:, None], totals], axis=1)
    fits = jnp.all(sizes <= bounds, axis=(1, 2))
    choice = len(tiers) - 1 - jnp.sum(fits.astype(jnp.int32))
    inputs = list_inputs(tile_cols, lists, ranks, rows, here, core, loc)
    runs = [run(caps) for caps in tiers]
    partial = lax.switch(choice, runs, mine, other, index, inputs)

    width = tile // 2
    keep = lax.dynamic_slice_in_dim(partial, core * width, width, 1)
    give = lax.dynamic_slice_in_dim(partial, (1 - core) * width, width, 1)
    return keep + swap_cores(give)


def solution(mesh):
    return jax.shard_map(
        body,
        mesh=mesh,
        in_specs=(P("row", "rep", None, None), P()),
        out_specs=P("row", "rep"),
        check_vma=False,
    )
```
